32 devices in a mesh: blk: 16 (over z, y, x), grp: 2 (over core).
Axes of the slice: x: 2, y: 2, z: 4, core: 2. Of those that a mesh axis runs over, the one named last changes fastest.
Arguments:
- returns: float32 [512, 8192], P(None, ('blk', 'grp')), may hold values from -200 to 200
Outputs:
- correlation: bfloat16 [8192, 8192], P(('blk', 'grp'))
The draws below stay inside these ranges and needn't reach their ends.
All inputs are finite; a program needn't handle non-finite values.
Results may differ from the reference program's by a relative error of at most 0.0034.
Values may be sent and summed in bfloat16 or wider, within the bound.
No kernel may reach another device: no remote copies, remote signals or barrier semaphores. Data moves between devices by JAX's collectives and lax.ppermute only.
A program may use at most 128 MiB of HBM per device.

```python
import math
import jax
import jax.numpy as jnp
from jax import lax

SER_DEV = 256
BARS = 512
SERIES = 8192


def draw_returns(key, part):
    subkeys = jax.random.split(key, 4)
    factor = jnp.clip(jax.random.normal(subkeys[0], (BARS, 1), jnp.float32), -4.0, 4.0)
    position = jnp.arange(SERIES, dtype=jnp.float32)[None, :] / SERIES
    loading = 0.5 + position + 0.3 * jnp.clip(jax.random.normal(subkeys[1], (1, SERIES), jnp.float32), -4.0, 4.0)
    volatility = jnp.exp(jax.random.uniform(subkeys[2], (1, SERIES), jnp.float32, math.log(0.3), math.log(3.0)))
    specific = 0.7 * jnp.clip(jax.random.normal(subkeys[3], (BARS, SERIES), jnp.float32), -4.0, 4.0)
    return (volatility * (factor * loading + specific)).astype(jnp.float32)


def setup_inputs(seed: int = 0) -> dict:
    arg_keys = jax.random.split(jax.random.key(seed), 2)
    returns = draw_returns(jax.random.fold_in(arg_keys[1], 71), 0)
    return {"returns": returns}


def reference(returns):
    market = lax.optimization_barrier(jnp.mean(returns, axis=1, keepdims=True))
    excess = returns - market
    deviation = excess - lax.optimization_barrier(jnp.mean(excess, axis=0, keepdims=True))
    inverse = lax.rsqrt(lax.optimization_barrier(jnp.mean(deviation * deviation, axis=0, keepdims=True)) + 1e-06) / math.sqrt(BARS)
    zscores = (deviation * inverse).astype(jnp.bfloat16)
    blocks = SERIES // SER_DEV
    columns = jnp.arange(SERIES, dtype=jnp.int32) // SER_DEV

    def row_block(row_index):
        block_rows = lax.dynamic_slice_in_dim(zscores, (row_index * SER_DEV).astype(jnp.int32), SER_DEV, 1)
        products = lax.dot_general(block_rows, zscores, (((0,), (0,)), ((), ())), preferred_element_type=jnp.float32)
        return jnp.where(columns[None, :] >= row_index, products, jnp.float32(0.0)).astype(jnp.bfloat16)
    stacked = lax.map(row_block, jnp.arange(blocks, dtype=jnp.int32))
    return stacked.reshape(SERIES, SERIES)
```

```python
import functools
import math

import jax
import jax.numpy as jnp
from jax import lax
from jax.experimental import pallas as pl
from jax.experimental.pallas import tpu as pltpu
from jax.sharding import PartitionSpec as P

AXES = ("blk", "grp")


def tiles_kernel(count, aliased, cols_ref, zt_ref, *refs):
    blocks = refs[:count]
    out = refs[count + aliased]
    tile, sems = refs[count + aliased + 1 :]
    width = blocks[0].shape[1]
    me = cols_ref[count]
    copies = []
    for n in range(count):
        col = cols_ref[n]

        @pl.when(col >= me)
        def _():
            tile[n] = jnp.dot(
                zt_ref[...], blocks[n][...], preferred_element_type=jnp.float32
            ).astype(tile.dtype)

        @pl.when(col < me)
        def _():
            tile[n] = jnp.zeros(tile.shape[1:], tile.dtype)

        copy = pltpu.make_async_copy(
            tile.at[n],
            out.at[:, pl.ds(pl.multiple_of(col * width, width), width)],
            sems.at[n],
        )
        copy.start()
        copies.append(copy)
    for copy in copies:
        copy.wait()


def tiles(zt, blocks, cols, me, total, prev):
    count = len(blocks)
    rows, depth = zt.shape
    width = blocks[0].shape[1]
    vm = pl.BlockSpec(memory_space=pltpu.VMEM)
    anyspec = pl.BlockSpec(memory_space=pl.ANY)
    aliased = prev is not None
    scalars = jnp.stack([*cols, me]).astype(jnp.int32)
    return pl.pallas_call(
        functools.partial(tiles_kernel, count, int(aliased)),
        out_shape=jax.ShapeDtypeStruct((rows, total), jnp.bfloat16),
        in_specs=[pl.BlockSpec(memory_space=pltpu.SMEM), vm]
        + [vm] * count
        + [anyspec] * int(aliased),
        out_specs=anyspec,
        scratch_shapes=[
            pltpu.VMEM((count, rows, width), jnp.bfloat16),
            pltpu.SemaphoreType.DMA((count,)),
        ],
        input_output_aliases={2 + count: 0} if aliased else {},
        cost_estimate=pl.CostEstimate(
            flops=2 * count * rows * depth * width,
            bytes_accessed=2 * count * (depth * width + rows * width),
            transcendentals=0,
        ),
        name=f"tiles_{count}",
    )(scalars, zt, *blocks, *([prev] if aliased else []))


def shards(returns):
    bar_count, series_dev = returns.shape
    blk, grp = (lax.axis_size(a) for a in AXES)
    devices = blk * grp
    b = lax.axis_index("blk")
    g = lax.axis_index("grp")
    me = b * grp + g
    summed = jnp.sum(returns, axis=1)
    parts = lax.all_to_all(
        jnp.broadcast_to(summed[None], (devices, bar_count)), AXES, 0, 0, tiled=True
    )
    market = jnp.sum(parts, axis=0) / (series_dev * devices)
    excess = returns - market[:, None]
    deviation = excess - jnp.mean(excess, axis=0, keepdims=True)
    inverse = lax.rsqrt(jnp.mean(deviation * deviation, axis=0, keepdims=True) + 1e-06) / math.sqrt(
        bar_count
    )
    z = (deviation * inverse).astype(jnp.bfloat16)
    zt = z.T
    total = series_dev * devices
    depth = blk // 4
    have = {(0, "O"): z}

    def up(x):
        return lax.ppermute(x, "blk", [(i, (i - 4) % blk) for i in range(blk)])

    def cross(x, bit):
        return lax.ppermute(x, "blk", [(i, i ^ bit) for i in range(blk)])

    def share(x):
        return [x] + [
            lax.ppermute(x, "grp", [(i, (i - j) % grp) for i in range(grp)])
            for j in range(1, grp)
        ]

    moves = schedule(depth)
    bits = {"O": 0, "X": 1, "Y": 2, "D": 3}
    out = None
    pending = [(0, "O")]
    for number, step in enumerate(moves):
        new = {}
        for link, key in step:
            k, d = key
            if link == "z":
                new[key] = up(have[(k - 1, d)])
            elif link == "x":
                new[key] = cross(have[(k, {"X": "O", "D": "Y"}[d])], 1)
            else:
                new[key] = cross(have[(k, {"Y": "O", "D": "X"}[d])], 2)
        if number in FLUSH or number == len(moves):
            out = flush(zt, have, pending, bits, b, g, me, blk, grp, total, out, share)
            pending = []
        have.update(new)
        pending += list(new)
    return flush(zt, have, pending, bits, b, g, me, blk, grp, total, out, share)


FLUSH = (2, 4)


def flush(zt, have, keys, bits, b, g, me, blk, grp, total, out, share):
    blocks, cols = [], []
    for k, d in keys:
        col = lax.rem(b + 4 * k, blk) ^ bits[d]
        for j, x in enumerate(share(have[(k, d)])):
            blocks.append(x)
            cols.append(col * grp + lax.rem(g + j, grp))
    return tiles(zt, blocks, cols, me, total, out)


def schedule(depth):
    lanes = {
        "z": [(k, "O") for k in range(1, depth)] + [(k, "D") for k in range(2, depth)],
        "x": [(k, "X") for k in range(depth)],
        "y": [(k, "Y") for k in range(depth)],
    }
    lanes["x"].insert(min(3, depth), (0, "D"))
    if depth > 1:
        lanes["y"].insert(2, (1, "D"))
    have = {(0, "O")}
    steps = []
    while any(lanes.values()):
        step = []
        for link, queue in lanes.items():
            if not queue:
                continue
            k, d = queue[0]
            need = {
                "z": (k - 1, d),
                "x": (k, {"X": "O", "D": "Y"}.get(d)),
                "y": (k, {"Y": "O", "D": "X"}.get(d)),
            }[link]
            if need in have:
                step.append((link, queue.pop(0)))
        have.update(key for _, key in step)
        steps.append(step)
    return steps


def solution(mesh):
    spec = P(None, AXES)
    return jax.shard_map(
        shards, mesh=mesh, in_specs=(spec,), out_specs=P(AXES, None), check_vma=False
    )


if __name__ == "__main__":
    for s in schedule(4):
        print(s)
```

```python
import functools
import math

import jax
import jax.numpy as jnp
from jax import lax
from jax.experimental import pallas as pl
from jax.experimental.pallas import tpu as pltpu
from jax.sharding import PartitionSpec as P


AXES = ("blk", "grp")
PLACES = {"O": 0, "X": 1, "Y": 2, "D": 3}
VMEM = pl.BlockSpec(memory_space=pltpu.VMEM)
ANY = pl.BlockSpec(memory_space=pl.ANY)
SMALL = pltpu.CompilerParams(vmem_limit_bytes=12 << 20)


def sums_kernel(r_ref, out_ref):
    summed = lax.dot_general(
        jnp.ones((8, r_ref.shape[1]), jnp.float32),
        r_ref[...],
        (((1,), (1,)), ((), ())),
        precision=lax.Precision.HIGHEST,
        preferred_element_type=jnp.float32,
    )
    for n in range(out_ref.shape[0]):
        out_ref[n] = summed[:1]


def sums(returns, devices):
    bars, width = returns.shape
    return pl.pallas_call(
        sums_kernel,
        out_shape=jax.ShapeDtypeStruct((devices, 1, bars), jnp.float32),
        in_specs=[VMEM],
        out_specs=VMEM,
        compiler_params=SMALL,
        cost_estimate=pl.CostEstimate(
            flops=bars * width, bytes_accessed=4 * bars * width, transcendentals=0
        ),
        name="sums",
    )(returns)


def stats_kernel(series, r_ref, parts_ref, z_ref, zt_ref):
    bars, width = r_ref.shape
    summed = jnp.sum(parts_ref[...], axis=0) * (1.0 / series)
    market = lax.dot_general(
        summed,
        jnp.ones((1, width), jnp.float32),
        (((0,), (0,)), ((), ())),
        precision=lax.Precision.HIGHEST,
        preferred_element_type=jnp.float32,
    )
    excess = r_ref[...] - market
    deviation = excess - jnp.sum(excess, axis=0, keepdims=True) * (1.0 / bars)
    variance = jnp.sum(deviation * deviation, axis=0, keepdims=True) * (1.0 / bars)
    z = deviation * (lax.rsqrt(variance + 1e-06) * (1.0 / math.sqrt(bars)))
    z_ref[...] = z.astype(jnp.bfloat16)
    zt_ref[...] = z.T.astype(jnp.bfloat16)


def stats(returns, parts, series):
    bars, width = returns.shape
    return pl.pallas_call(
        functools.partial(stats_kernel, series),
        out_shape=(
            jax.ShapeDtypeStruct((bars, width), jnp.bfloat16),
            jax.ShapeDtypeStruct((width, bars), jnp.bfloat16),
        ),
        in_specs=[VMEM, VMEM],
        out_specs=(VMEM, VMEM),
        compiler_params=SMALL,
        cost_estimate=pl.CostEstimate(
            flops=8 * bars * width, bytes_accessed=8 * bars * width, transcendentals=width
        ),
        name="stats",
    )(returns, parts)


def tiles_kernel(cores, keys, stack_keys, aliased, *refs):
    count = len(keys)
    blk = lax.axis_size("blk")
    b, g = (lax.axis_index(a) for a in AXES)
    refs = list(refs)
    zts = [refs.pop(0) for _ in range(cores)]
    blocks = [refs.pop(0) for _ in range(count)]
    stacks = [refs.pop(0) for _ in range(cores - 1 if stack_keys else 0)]
    if aliased:
        refs.pop(0)
    out = refs.pop(0)
    sends = [refs.pop(0) for _ in range(cores - 1)] if count else []
    tile, sems = refs
    copies = []

    def place(src, col):
        width = src.shape[1]
        copy = pltpu.make_async_copy(
            src, out.at[:, pl.ds(pl.multiple_of(col * width, width), width)], sems.at[len(copies)]
        )
        copy.start()
        copies.append(copy)

    def column(key, lane):
        k, d = key
        return (lax.rem(b + 4 * k, blk) ^ PLACES[d]) * cores + lane

    for j, stack in enumerate(stacks, 1):
        for n, key in enumerate(stack_keys):
            place(stack.at[n], column(key, lax.rem(g + cores - j, cores)))

    def product(dst, n, j):
        live = column(keys[n], g) >= b * cores + lax.rem(g + j, cores)

        @pl.when(live)
        def _():
            dst[n] = jnp.dot(
                zts[j][...], blocks[n][...], preferred_element_type=jnp.float32
            ).astype(dst.dtype)

        @pl.when(jnp.logical_not(live))
        def _():
            dst[n] = jnp.zeros(dst.shape[1:], dst.dtype)

    for n in range(count):
        product(tile, n, 0)
        place(tile.at[n], column(keys[n], g))
    for j in range(1, cores):
        for n in range(count):
            product(sends[j - 1], n, j)
    for copy in copies:
        copy.wait()


def tiles(zts, keys, blocks, stack_keys, stacks, total, prev):
    cores, count = len(zts), len(blocks)
    height, depth = zts[0].shape
    aliased = int(prev is not None)
    placed = len(stacks) * len(stack_keys)
    out_shape = [jax.ShapeDtypeStruct((height, total), jnp.bfloat16)]
    out_specs = [ANY]
    if count:
        out_shape += [jax.ShapeDtypeStruct((count, height, height), jnp.bfloat16)] * (cores - 1)
        out_specs += [VMEM] * (cores - 1)
    got = pl.pallas_call(
        functools.partial(tiles_kernel, cores, keys, stack_keys, aliased),
        out_shape=out_shape,
        in_specs=[VMEM] * (cores + count + len(stacks)) + [ANY] * aliased,
        out_specs=out_specs,
        scratch_shapes=[
            pltpu.VMEM((max(count, 1), height, height), jnp.bfloat16),
            pltpu.SemaphoreType.DMA((count + placed,)),
        ],
        input_output_aliases={cores + count + len(stacks): 0} if aliased else {},
        compiler_params=SMALL,
        cost_estimate=pl.CostEstimate(
            flops=2 * max(count, 1) * cores * height * depth * height,
            bytes_accessed=2 * count * (depth * height + cores * height * height),
            transcendentals=0,
        ),
    )(*zts, *blocks, *stacks, *([prev] if aliased else []))
    return got[0], list(got[1:])


def schedule(depth):
    lanes = {
        "z": [(k, "O") for k in range(1, depth)] + [(k, "D") for k in range(2, depth)],
        "x": [(k, "X") for k in range(depth)],
        "y": [(k, "Y") for k in range(depth)],
    }
    lanes["x"].insert(min(3, depth), (0, "D"))
    if depth > 1:
        lanes["y"].insert(2, (1, "D"))
    have = {(0, "O")}
    steps = []
    while any(lanes.values()):
        step = []
        for link, queue in lanes.items():
            if queue and source(link, queue[0]) in have:
                step.append((link, queue.pop(0)))
        have.update(key for _, key in step)
        steps.append(step)
    return steps


def source(link, key):
    k, d = key
    if link == "z":
        return (k - 1, d)
    return (k, {"x": {"X": "O", "D": "Y"}, "y": {"Y": "O", "D": "X"}}[link].get(d))


def hop(x, link, blk):
    move = {"z": lambda i: (i - 4) % blk, "x": lambda i: i ^ 1, "y": lambda i: i ^ 2}[link]
    return lax.ppermute(x, "blk", [(i, move(i)) for i in range(blk)])


def turn(x, j, grp):
    return lax.ppermute(x, "grp", [(i, (i - j) % grp) for i in range(grp)])


def shards(steps, returns):
    _, width = returns.shape
    blk, grp = (lax.axis_size(a) for a in AXES)
    devices = blk * grp
    total = width * devices
    parts = lax.all_to_all(sums(returns, devices), AXES, 0, 0, tiled=True)
    z, zt = stats(returns, parts, total)
    have = {(0, "O"): z}
    zts, out, stacks, stack_keys = [zt], None, [], []

    def consume(keys):
        nonlocal out, stacks, stack_keys
        out, sends = tiles(zts, keys, [have[key] for key in keys], stack_keys, stacks, total, out)
        stacks, stack_keys = [], keys
        for j, sent in enumerate(sends, 1):
            stacks.append(turn(sent, grp - j, grp))

    ready = [(0, "O")]
    for number, step in enumerate(steps):
        arrived = {}
        for link, key in step:
            arrived[key] = hop(have[source(link, key)], link, blk)
        if not number:
            for j in range(1, grp):
                zts.append(turn(zt, j, grp))
        consume(ready)
        have.update(arrived)
        ready = list(arrived)
    consume(ready)
    consume([])
    return out


def solution(mesh):
    blk, _ = (mesh.shape[a] for a in AXES)
    steps = schedule(blk // 4)
    return jax.shard_map(
        functools.partial(shards, steps),
        mesh=mesh,
        in_specs=(P(None, AXES),),
        out_specs=P(AXES, None),
        check_vma=False,
    )
```

```python
import functools
import math

import jax
import jax.numpy as jnp
from jax import lax
from jax.experimental import pallas as pl
from jax.experimental.pallas import tpu as pltpu
from jax.sharding import PartitionSpec as P


AXES = ("blk", "grp")
PLACES = {"O": 0, "X": 1, "Y": 2, "D": 3}
VMEM = pl.BlockSpec(memory_space=pltpu.VMEM)
ANY = pl.BlockSpec(memory_space=pl.ANY)
SMALL = pltpu.CompilerParams(vmem_limit_bytes=12 << 20)


def sums_kernel(r_ref, out_ref):
    summed = lax.dot_general(
        jnp.ones((8, r_ref.shape[1]), jnp.float32),
        r_ref[...],
        (((1,), (1,)), ((), ())),
        precision=lax.Precision.HIGHEST,
        preferred_element_type=jnp.float32,
    )
    for n in range(out_ref.shape[0]):
        out_ref[n] = summed[:1]


def sums(returns, devices):
    bars, width = returns.shape
    return pl.pallas_call(
        sums_kernel,
        out_shape=jax.ShapeDtypeStruct((devices, 1, bars), jnp.float32),
        in_specs=[VMEM],
        out_specs=VMEM,
        compiler_params=SMALL,
        cost_estimate=pl.CostEstimate(
            flops=bars * width, bytes_accessed=4 * bars * width, transcendentals=0
        ),
        name="sums",
    )(returns)


def stats_kernel(series, r_ref, parts_ref, z_ref, zt_ref):
    bars, width = r_ref.shape
    summed = jnp.sum(parts_ref[...], axis=0) * (1.0 / series)
    market = lax.dot_general(
        summed,
        jnp.ones((1, width), jnp.float32),
        (((0,), (0,)), ((), ())),
        precision=lax.Precision.HIGHEST,
        preferred_element_type=jnp.float32,
    )
    excess = r_ref[...] - market
    deviation = excess - jnp.sum(excess, axis=0, keepdims=True) * (1.0 / bars)
    variance = jnp.sum(deviation * deviation, axis=0, keepdims=True) * (1.0 / bars)
    z = deviation * (lax.rsqrt(variance + 1e-06) * (1.0 / math.sqrt(bars)))
    z_ref[...] = z.astype(jnp.bfloat16)
    zt_ref[...] = z.T.astype(jnp.bfloat16)


def stats(returns, parts, series):
    bars, width = returns.shape
    return pl.pallas_call(
        functools.partial(stats_kernel, series),
        out_shape=(
            jax.ShapeDtypeStruct((bars, width), jnp.bfloat16),
            jax.ShapeDtypeStruct((width, bars), jnp.bfloat16),
        ),
        in_specs=[VMEM, VMEM],
        out_specs=(VMEM, VMEM),
        compiler_params=SMALL,
        cost_estimate=pl.CostEstimate(
            flops=8 * bars * width, bytes_accessed=8 * bars * width, transcendentals=width
        ),
        name="stats",
    )(returns, parts)


def tiles_kernel(cores, keys, stack_keys, aliased, own, others, *refs):
    count = len(keys)
    blk = lax.axis_size("blk")
    b, g = (lax.axis_index(a) for a in AXES)
    refs = list(refs)
    zts = [refs.pop(0) for _ in range(cores)]
    blocks = [refs.pop(0) for _ in range(count)]
    stacks = [refs.pop(0) for _ in range(cores - 1 if stack_keys else 0)]
    if aliased:
        refs.pop(0)
    out = refs.pop(0) if own or stacks else None
    sends = [refs.pop(0) for _ in range(cores - 1)] if others else []
    tile, sems = refs
    copies = []

    def place(src, col):
        width = src.shape[1]
        copy = pltpu.make_async_copy(
            src, out.at[:, pl.ds(pl.multiple_of(col * width, width), width)], sems.at[len(copies)]
        )
        copy.start()
        copies.append(copy)

    def column(key, lane):
        k, d = key
        return (lax.rem(b + 4 * k, blk) ^ PLACES[d]) * cores + lane

    for j, stack in enumerate(stacks, 1):
        for n, key in enumerate(stack_keys):
            place(stack.at[n], column(key, lax.rem(g + cores - j, cores)))

    def product(dst, n, j):
        live = column(keys[n], g) >= b * cores + lax.rem(g + j, cores)

        @pl.when(live)
        def _():
            dst[n] = jnp.dot(
                zts[j][...], blocks[n][...], preferred_element_type=jnp.float32
            ).astype(dst.dtype)

        @pl.when(jnp.logical_not(live))
        def _():
            dst[n] = jnp.zeros(dst.shape[1:], dst.dtype)

    if own:
        for n in range(count):
            product(tile, n, 0)
            place(tile.at[n], column(keys[n], g))
    for j, send in enumerate(sends, 1):
        for n in range(count):
            product(send, n, j)
    for copy in copies:
        copy.wait()


def tiles(zts, keys, blocks, stack_keys, stacks, total, prev, own=True, others=True):
    cores, count = len(zts), len(blocks)
    height, depth = zts[0].shape
    own, others = own and count > 0, others and count > 0
    writes = own or stacks
    aliased = int(bool(writes) and prev is not None)
    placed = len(stacks) * len(stack_keys)
    out_shape, out_specs = [], []
    if writes:
        out_shape += [jax.ShapeDtypeStruct((height, total), jnp.bfloat16)]
        out_specs += [ANY]
    if others:
        out_shape += [jax.ShapeDtypeStruct((count, height, height), jnp.bfloat16)] * (cores - 1)
        out_specs += [VMEM] * (cores - 1)
    got = pl.pallas_call(
        functools.partial(tiles_kernel, cores, keys, stack_keys, aliased, own, others),
        out_shape=out_shape,
        in_specs=[VMEM] * (cores + count + len(stacks)) + [ANY] * aliased,
        out_specs=out_specs,
        scratch_shapes=[
            pltpu.VMEM((max(count * own, 1), height, height), jnp.bfloat16),
            pltpu.SemaphoreType.DMA((max(count * own + placed, 1),)),
        ],
        input_output_aliases={cores + count + len(stacks): 0} if aliased else {},
        compiler_params=SMALL,
        cost_estimate=pl.CostEstimate(
            flops=2 * max(count, 1) * (own + others) * height * depth * height + 1000,
            bytes_accessed=2 * count * (depth * height + cores * height * height),
            transcendentals=0,
        ),
    )(*zts, *blocks, *stacks, *([prev] if aliased else []))
    got = list(got)
    return got.pop(0) if writes else prev, got


def schedule(depth):
    lanes = {
        "z": [(k, "O") for k in range(1, depth)] + [(k, "D") for k in range(2, depth)],
        "x": [(k, "X") for k in range(depth)],
        "y": [(k, "Y") for k in range(depth)],
    }
    lanes["x"].insert(min(3, depth), (0, "D"))
    if depth > 1:
        lanes["y"].insert(2, (1, "D"))
    have = {(0, "O")}
    steps = []
    while any(lanes.values()):
        step = []
        for link, queue in lanes.items():
            if queue and source(link, queue[0]) in have:
                step.append((link, queue.pop(0)))
        have.update(key for _, key in step)
        steps.append(step)
    return steps


def source(link, key):
    k, d = key
    if link == "z":
        return (k - 1, d)
    return (k, {"x": {"X": "O", "D": "Y"}, "y": {"Y": "O", "D": "X"}}[link].get(d))


def climb(k, depth, grp):
    top = depth - k + 1
    rest = depth - top
    pairs = []
    for p in range(depth):
        for i in range(4):
            for c in range(grp):
                if p < top:
                    to = (p - 1) % top, i, c
                elif rest > 1:
                    to = top + (p - top + 1) % rest, i, c
                else:
                    to = p, i, (c + 1) % grp
                pairs.append(((p * 4 + i) * grp + c, (to[0] * 4 + to[1]) * grp + to[2]))
    return pairs


def hop(x, link, key, blk, grp):
    if link == "z":
        return lax.ppermute(x, AXES, climb(key[0], blk // 4, grp))
    bit = {"x": 1, "y": 2}[link]
    return lax.ppermute(x, "blk", [(i, i ^ bit) for i in range(blk)])


def turn(x, j, grp):
    return lax.ppermute(x, "grp", [(i, (i - j) % grp) for i in range(grp)])


def shards(steps, returns):
    _, width = returns.shape
    blk, grp = (lax.axis_size(a) for a in AXES)
    devices = blk * grp
    total = width * devices
    parts = lax.all_to_all(sums(returns, devices), AXES, 0, 0, tiled=True)
    z, zt = stats(returns, parts, total)
    have = {(0, "O"): z}
    zts, out, stacks, stack_keys = [zt], None, [], []

    def consume(keys, split=False):
        nonlocal out, stacks, stack_keys
        blocks = [have[key] for key in keys]
        if split:
            _, sends = tiles(zts, keys, blocks, (), [], total, None, own=False)
            out, _ = tiles(zts, keys, blocks, stack_keys, stacks, total, out, others=False)
        else:
            out, sends = tiles(zts, keys, blocks, stack_keys, stacks, total, out)
        stacks, stack_keys = [], keys
        for j, sent in enumerate(sends, 1):
            stacks.append(turn(sent, grp - j, grp))

    ready = [(0, "O")]
    for number, step in enumerate(steps):
        arrived = {}
        for link, key in step:
            arrived[key] = hop(have[source(link, key)], link, key, blk, grp)
        if not number:
            for j in range(1, grp):
                zts.append(turn(zt, j, grp))
        consume(ready)
        have.update(arrived)
        ready = list(arrived)
    consume(ready, split=grp > 1)
    consume([])
    return out


def solution(mesh):
    blk, _ = (mesh.shape[a] for a in AXES)
    steps = schedule(blk // 4)
    return jax.shard_map(
        functools.partial(shards, steps),
        mesh=mesh,
        in_specs=(P(None, AXES),),
        out_specs=P(AXES, None),
        check_vma=False,
    )
```

```python
import functools
import math

import jax
import jax.numpy as jnp
from jax import lax
from jax.experimental import pallas as pl
from jax.experimental.pallas import tpu as pltpu
from jax.sharding import PartitionSpec as P


AXES = ("blk", "grp")
PLACES = {"O": 0, "X": 1, "Y": 2, "D": 3}
PIECES = 2
VMEM = pl.BlockSpec(memory_space=pltpu.VMEM)
ANY = pl.BlockSpec(memory_space=pl.ANY)
SMALL = pltpu.CompilerParams(vmem_limit_bytes=12 << 20)


def sums_kernel(r_ref, out_ref):
    summed = lax.dot_general(
        jnp.ones((8, r_ref.shape[1]), jnp.float32),
        r_ref[...],
        (((1,), (1,)), ((), ())),
        precision=lax.Precision.HIGHEST,
        preferred_element_type=jnp.float32,
    )
    for n in range(out_ref.shape[0]):
        out_ref[n] = summed[:1]


def sums(returns, devices):
    bars, width = returns.shape
    return pl.pallas_call(
        sums_kernel,
        out_shape=jax.ShapeDtypeStruct((devices, 1, bars), jnp.float32),
        in_specs=[VMEM],
        out_specs=VMEM,
        compiler_params=SMALL,
        cost_estimate=pl.CostEstimate(
            flops=bars * width, bytes_accessed=4 * bars * width, transcendentals=0
        ),
        name="sums",
    )(returns)


def stats_kernel(series, r_ref, parts_ref, zt_ref, *z_refs):
    bars, width = r_ref.shape
    summed = jnp.sum(parts_ref[...], axis=0) * (1.0 / series)
    market = lax.dot_general(
        summed,
        jnp.ones((1, width), jnp.float32),
        (((0,), (0,)), ((), ())),
        precision=lax.Precision.HIGHEST,
        preferred_element_type=jnp.float32,
    )
    excess = r_ref[...] - market
    deviation = excess - jnp.sum(excess, axis=0, keepdims=True) * (1.0 / bars)
    variance = jnp.sum(deviation * deviation, axis=0, keepdims=True) * (1.0 / bars)
    z = deviation * (lax.rsqrt(variance + 1e-06) * (1.0 / math.sqrt(bars)))
    piece = bars // len(z_refs)
    for n, z_ref in enumerate(z_refs):
        z_ref[...] = z[n * piece : (n + 1) * piece].astype(jnp.bfloat16)
    zt_ref[...] = z.T.astype(jnp.bfloat16)


def stats(returns, parts, series):
    bars, width = returns.shape
    return pl.pallas_call(
        functools.partial(stats_kernel, series),
        out_shape=(
            jax.ShapeDtypeStruct((width, bars), jnp.bfloat16),
            *[jax.ShapeDtypeStruct((bars // PIECES, width), jnp.bfloat16)] * PIECES,
        ),
        in_specs=[VMEM, VMEM],
        out_specs=(VMEM,) * (1 + PIECES),
        compiler_params=SMALL,
        cost_estimate=pl.CostEstimate(
            flops=8 * bars * width, bytes_accessed=8 * bars * width, transcendentals=width
        ),
        name="stats",
    )(returns, parts)


def tiles_kernel(cores, keys, stack_keys, aliased, own, others, *refs):
    count = len(keys)
    blk = lax.axis_size("blk")
    b, g = (lax.axis_index(a) for a in AXES)
    refs = list(refs)
    zts = [refs.pop(0) for _ in range(cores)]
    blocks = [[refs.pop(0) for _ in range(PIECES)] for _ in range(count)]
    stacks = [refs.pop(0) for _ in range(cores - 1 if stack_keys else 0)]
    if aliased:
        refs.pop(0)
    out = refs.pop(0) if own or stacks else None
    sends = [refs.pop(0) for _ in range(cores - 1)] if others else []
    tile, sems = refs
    copies = []

    def place(src, col):
        width = src.shape[1]
        copy = pltpu.make_async_copy(
            src, out.at[:, pl.ds(pl.multiple_of(col * width, width), width)], sems.at[len(copies)]
        )
        copy.start()
        copies.append(copy)

    def column(key, lane):
        k, d = key
        return (lax.rem(b + 4 * k, blk) ^ PLACES[d]) * cores + lane

    for j, stack in enumerate(stacks, 1):
        for n, key in enumerate(stack_keys):
            place(stack.at[n], column(key, lax.rem(g + cores - j, cores)))

    def product(dst, n, j):
        live = column(keys[n], g) >= b * cores + lax.rem(g + j, cores)

        @pl.when(live)
        def _():
            bars = blocks[n][0].shape[0]
            dst[n] = sum(
                jnp.dot(
                    zts[j][:, m * bars : (m + 1) * bars],
                    piece[...],
                    preferred_element_type=jnp.float32,
                )
                for m, piece in enumerate(blocks[n])
            ).astype(dst.dtype)

        @pl.when(jnp.logical_not(live))
        def _():
            dst[n] = jnp.zeros(dst.shape[1:], dst.dtype)

    if own:
        for n in range(count):
            product(tile, n, 0)
            place(tile.at[n], column(keys[n], g))
    for j, send in enumerate(sends, 1):
        for n in range(count):
            product(send, n, j)
    for copy in copies:
        copy.wait()


def tiles(zts, keys, blocks, stack_keys, stacks, total, prev, own=True, others=True):
    cores, count = len(zts), len(blocks)
    height, depth = zts[0].shape
    own, others = own and count > 0, others and count > 0
    writes = own or stacks
    aliased = int(bool(writes) and prev is not None)
    placed = len(stacks) * len(stack_keys)
    out_shape, out_specs = [], []
    if writes:
        out_shape += [jax.ShapeDtypeStruct((height, total), jnp.bfloat16)]
        out_specs += [ANY]
    if others:
        out_shape += [jax.ShapeDtypeStruct((count, height, height), jnp.bfloat16)] * (cores - 1)
        out_specs += [VMEM] * (cores - 1)
    got = pl.pallas_call(
        functools.partial(tiles_kernel, cores, keys, stack_keys, aliased, own, others),
        out_shape=out_shape,
        in_specs=[VMEM] * (cores + count * PIECES + len(stacks)) + [ANY] * aliased,
        out_specs=out_specs,
        scratch_shapes=[
            pltpu.VMEM((max(count * own, 1), height, height), jnp.bfloat16),
            pltpu.SemaphoreType.DMA((max(count * own + placed, 1),)),
        ],
        input_output_aliases={cores + count * PIECES + len(stacks): 0} if aliased else {},
        compiler_params=SMALL,
        cost_estimate=pl.CostEstimate(
            flops=2 * max(count, 1) * (own + others) * height * depth * height + 1000,
            bytes_accessed=2 * count * (depth * height + cores * height * height),
            transcendentals=0,
        ),
    )(*zts, *(piece for block in blocks for piece in block), *stacks, *([prev] if aliased else []))
    got = list(got)
    return got.pop(0) if writes else prev, got


def schedule(depth):
    lanes = {
        "z": [(k, "O") for k in range(1, depth)] + [(k, "D") for k in range(2, depth)],
        "x": [(k, "X") for k in range(depth)],
        "y": [(k, "Y") for k in range(depth)],
    }
    lanes["x"].insert(min(3, depth), (0, "D"))
    if depth > 1:
        lanes["y"].insert(2, (1, "D"))
    have = {(0, "O")}
    steps = []
    while any(lanes.values()):
        step = []
        for link, queue in lanes.items():
            if queue and source(link, queue[0]) in have:
                step.append((link, queue.pop(0)))
        have.update(key for _, key in step)
        steps.append(step)
    return steps


def source(link, key):
    k, d = key
    if link == "z":
        return (k - 1, d)
    return (k, {"x": {"X": "O", "D": "Y"}, "y": {"Y": "O", "D": "X"}}[link].get(d))


def climb(k, depth, grp):
    top = depth - k + 1
    rest = depth - top
    pairs = []
    for p in range(depth):
        for i in range(4):
            for c in range(grp):
                if p < top:
                    to = (p - 1) % top, i, c
                elif rest > 1:
                    to = top + (p - top + 1) % rest, i, c
                else:
                    to = p, i, (c + 1) % grp
                pairs.append(((p * 4 + i) * grp + c, (to[0] * 4 + to[1]) * grp + to[2]))
    return pairs


def hop(x, link, key, blk, grp):
    if link == "z":
        return lax.ppermute(x, AXES, climb(key[0], blk // 4, grp))
    bit = {"x": 1, "y": 2}[link]
    return lax.ppermute(x, "blk", [(i, i ^ bit) for i in range(blk)])


def turn(x, j, grp):
    return lax.ppermute(x, "grp", [(i, (i - j) % grp) for i in range(grp)])


def shards(steps, returns):
    _, width = returns.shape
    blk, grp = (lax.axis_size(a) for a in AXES)
    devices = blk * grp
    total = width * devices
    parts = lax.all_to_all(sums(returns, devices), AXES, 0, 0, tiled=True)
    zt, *z = stats(returns, parts, total)
    have = {(0, "O"): z}
    zts, out, stacks, stack_keys = [zt], None, [], []

    def consume(keys, split=False):
        nonlocal out, stacks, stack_keys
        blocks = [have[key] for key in keys]
        if split:
            _, sends = tiles(zts, keys, blocks, (), [], total, None, own=False)
            out, _ = tiles(zts, keys, blocks, stack_keys, stacks, total, out, others=False)
        else:
            out, sends = tiles(zts, keys, blocks, stack_keys, stacks, total, out)
        stacks, stack_keys = [], keys
        for j, sent in enumerate(sends, 1):
            stacks.append(turn(sent, grp - j, grp))

    ready = [(0, "O")]
    for number, step in enumerate(steps):
        arrived = {key: [None] * PIECES for _, key in step}
        for n in range(PIECES):
            for link, key in step:
                arrived[key][n] = hop(have[source(link, key)][n], link, key, blk, grp)
        if number:
            consume(ready)
            ready = []
        else:
            for j in range(1, grp):
                zts.append(turn(zt, j, grp))
        have.update(arrived)
        ready += list(arrived)
    consume(ready, split=grp > 1)
    consume([])
    return out


def solution(mesh):
    blk, _ = (mesh.shape[a] for a in AXES)
    steps = schedule(blk // 4)
    return jax.shard_map(
        functools.partial(shards, steps),
        mesh=mesh,
        in_specs=(P(None, AXES),),
        out_specs=P(AXES, None),
        check_vma=False,
    )
```

```python
import functools
import math

import jax
import jax.numpy as jnp
from jax import lax
from jax.experimental import pallas as pl
from jax.experimental.pallas import tpu as pltpu
from jax.sharding import PartitionSpec as P


AXES = ("blk", "grp")
PLACES = {"O": 0, "X": 1, "Y": 2, "D": 3}
VMEM = pl.BlockSpec(memory_space=pltpu.VMEM)
ANY = pl.BlockSpec(memory_space=pl.ANY)
SMALL = pltpu.CompilerParams(vmem_limit_bytes=12 << 20)


def sums_kernel(r_ref, out_ref):
    summed = lax.dot_general(
        jnp.ones((8, r_ref.shape[1]), jnp.float32),
        r_ref[...],
        (((1,), (1,)), ((), ())),
        precision=lax.Precision.HIGHEST,
        preferred_element_type=jnp.float32,
    )
    for n in range(out_ref.shape[0]):
        out_ref[n] = summed[:1]


def sums(returns, devices):
    bars, width = returns.shape
    return pl.pallas_call(
        sums_kernel,
        out_shape=jax.ShapeDtypeStruct((devices, 1, bars), jnp.float32),
        in_specs=[VMEM],
        out_specs=VMEM,
        compiler_params=SMALL,
        cost_estimate=pl.CostEstimate(
            flops=bars * width, bytes_accessed=4 * bars * width, transcendentals=0
        ),
        name="sums",
    )(returns)


def stats_kernel(series, r_ref, parts_ref, z_ref, zt_ref):
    bars, width = r_ref.shape
    summed = jnp.sum(parts_ref[...], axis=0) * (1.0 / series)
    market = lax.dot_general(
        summed,
        jnp.ones((1, width), jnp.float32),
        (((0,), (0,)), ((), ())),
        precision=lax.Precision.HIGHEST,
        preferred_element_type=jnp.float32,
    )
    excess = r_ref[...] - market
    deviation = excess - jnp.sum(excess, axis=0, keepdims=True) * (1.0 / bars)
    variance = jnp.sum(deviation * deviation, axis=0, keepdims=True) * (1.0 / bars)
    z = deviation * (lax.rsqrt(variance + 1e-06) * (1.0 / math.sqrt(bars)))
    z_ref[...] = z.astype(jnp.bfloat16)
    zt_ref[...] = z.T.astype(jnp.bfloat16)


def stats(returns, parts, series):
    bars, width = returns.shape
    return pl.pallas_call(
        functools.partial(stats_kernel, series),
        out_shape=(
            jax.ShapeDtypeStruct((bars, width), jnp.bfloat16),
            jax.ShapeDtypeStruct((width, bars), jnp.bfloat16),
        ),
        in_specs=[VMEM, VMEM],
        out_specs=(VMEM, VMEM),
        compiler_params=SMALL,
        cost_estimate=pl.CostEstimate(
            flops=8 * bars * width, bytes_accessed=8 * bars * width, transcendentals=width
        ),
        name="stats",
    )(returns, parts)


def tiles_kernel(cores, keys, stack_keys, aliased, own, others, *refs):
    count = len(keys)
    blk = lax.axis_size("blk")
    b, g = (lax.axis_index(a) for a in AXES)
    refs = list(refs)
    zts = [refs.pop(0) for _ in range(cores)]
    blocks = [refs.pop(0) for _ in range(count)]
    stacks = [refs.pop(0) for _ in range(cores - 1 if stack_keys else 0)]
    if aliased:
        refs.pop(0)
    out = refs.pop(0) if own or stacks else None
    sends = [refs.pop(0) for _ in range(cores - 1)] if others else []
    tile, sems = refs
    copies = []

    def place(src, col):
        width = src.shape[1]
        copy = pltpu.make_async_copy(
            src, out.at[:, pl.ds(pl.multiple_of(col * width, width), width)], sems.at[len(copies)]
        )
        copy.start()
        copies.append(copy)

    def column(key, lane):
        k, d = key
        return (lax.rem(b + 4 * k, blk) ^ PLACES[d]) * cores + lane

    for j, stack in enumerate(stacks, 1):
        for n, key in enumerate(stack_keys):
            place(stack.at[n], column(key, lax.rem(g + cores - j, cores)))

    def product(dst, n, j):
        live = column(keys[n], g) >= b * cores + lax.rem(g + j, cores)

        @pl.when(live)
        def _():
            dst[n] = jnp.dot(
                zts[j][...], blocks[n][...], preferred_element_type=jnp.float32
            ).astype(dst.dtype)

        @pl.when(jnp.logical_not(live))
        def _():
            dst[n] = jnp.zeros(dst.shape[1:], dst.dtype)

    if own:
        for n in range(count):
            product(tile, n, 0)
            place(tile.at[n], column(keys[n], g))
    for j, send in enumerate(sends, 1):
        for n in range(count):
            product(send, n, j)
    for copy in copies:
        copy.wait()


def tiles(zts, keys, blocks, stack_keys, stacks, total, prev, own=True, others=True):
    cores, count = len(zts), len(blocks)
    height, depth = zts[0].shape
    own, others = own and count > 0, others and count > 0
    writes = own or stacks
    aliased = int(bool(writes) and prev is not None)
    placed = len(stacks) * len(stack_keys)
    out_shape, out_specs = [], []
    if writes:
        out_shape += [jax.ShapeDtypeStruct((height, total), jnp.bfloat16)]
        out_specs += [ANY]
    if others:
        out_shape += [jax.ShapeDtypeStruct((count, height, height), jnp.bfloat16)] * (cores - 1)
        out_specs += [VMEM] * (cores - 1)
    got = pl.pallas_call(
        functools.partial(tiles_kernel, cores, keys, stack_keys, aliased, own, others),
        out_shape=out_shape,
        in_specs=[VMEM] * (cores + count + len(stacks)) + [ANY] * aliased,
        out_specs=out_specs,
        scratch_shapes=[
            pltpu.VMEM((max(count * own, 1), height, height), jnp.bfloat16),
            pltpu.SemaphoreType.DMA((max(count * own + placed, 1),)),
        ],
        input_output_aliases={cores + count + len(stacks): 0} if aliased else {},
        compiler_params=SMALL,
        cost_estimate=pl.CostEstimate(
            flops=2 * max(count, 1) * (own + others) * height * depth * height + 1000,
            bytes_accessed=2 * count * (depth * height + cores * height * height),
            transcendentals=0,
        ),
    )(*zts, *blocks, *stacks, *([prev] if aliased else []))
    got = list(got)
    return got.pop(0) if writes else prev, got


TUNED = {
    4: (
        *("z1O", "x0X", "y0Y", ":0O", "z2O", "y1Y", "x1X", "y0D", ":1O,0X,0Y", "z3O", "x2X", "x1D"),
        *(":2O,1Y,1X", "y3Y", "z2Y", ":0D,3O", "z3X", "y2D", "x3D", ":2Y", ":2X,1D,3Y"),
        *(":2D,3X,3D",),
    )
}


def plan(depth):
    if depth in TUNED:
        key = lambda text: (int(text[:-1]), text[-1])
        return [
            (w[0], tuple(map(key, w[1:].split(","))) if w[0] == ":" else key(w[1:]))
            for w in TUNED[depth]
        ]
    lanes = {
        "z": [(k, "O") for k in range(1, depth)] + [(k, "D") for k in range(2, depth)],
        "x": [(k, "X") for k in range(depth)],
        "y": [(k, "Y") for k in range(depth)],
    }
    lanes["x"].insert(min(3, depth), (0, "D"))
    if depth > 1:
        lanes["y"].insert(2, (1, "D"))
    have = {(0, "O")}
    ready = ((0, "O"),)
    order = []
    while any(lanes.values()):
        step = []
        for link, queue in lanes.items():
            if queue and source(link, queue[0]) in have:
                step.append((link, queue.pop(0)))
        have.update(key for _, key in step)
        order += [*step, (":", ready)]
        ready = tuple(key for _, key in step)
    return [*order, (":", ready)]


def source(link, key):
    k, d = key
    if link == "z":
        return (k - 1, d)
    return (k, {"x": {"X": "O", "D": "Y"}, "y": {"Y": "O", "D": "X"}}[link].get(d))


def climb(k, depth, grp):
    top = depth - k + 1
    rest = depth - top
    pairs = []
    for p in range(depth):
        for i in range(4):
            for c in range(grp):
                if p < top:
                    to = (p - 1) % top, i, c
                elif rest > 1:
                    to = top + (p - top + 1) % rest, i, c
                else:
                    to = p, i, (c + 1) % grp
                pairs.append(((p * 4 + i) * grp + c, (to[0] * 4 + to[1]) * grp + to[2]))
    return pairs


def hop(x, link, key, blk, grp):
    if link == "z":
        return lax.ppermute(x, AXES, climb(key[0], blk // 4, grp))
    bit = {"x": 1, "y": 2}[link]
    return lax.ppermute(x, "blk", [(i, i ^ bit) for i in range(blk)])


def turn(x, j, grp):
    return lax.ppermute(x, "grp", [(i, (i - j) % grp) for i in range(grp)])


def shards(order, returns):
    _, width = returns.shape
    blk, grp = (lax.axis_size(a) for a in AXES)
    devices = blk * grp
    total = width * devices
    parts = lax.all_to_all(sums(returns, devices), AXES, 0, 0, tiled=True)
    z, zt = stats(returns, parts, total)
    have = {(0, "O"): z}
    zts, out, stacks, stack_keys = [zt], None, [], []

    def consume(keys, split=False):
        nonlocal out, stacks, stack_keys
        blocks = [have[key] for key in keys]
        if split:
            _, sends = tiles(zts, keys, blocks, (), [], total, None, own=False)
            out, _ = tiles(zts, keys, blocks, stack_keys, stacks, total, out, others=False)
        else:
            out, sends = tiles(zts, keys, blocks, stack_keys, stacks, total, out)
        stacks, stack_keys = [], keys
        for j, sent in enumerate(sends, 1):
            stacks.append(turn(sent, grp - j, grp))

    for number, (what, key) in enumerate(order):
        if what != ":":
            have[key] = hop(have[source(what, key)], what, key, blk, grp)
            continue
        if len(zts) < grp:
            for j in range(1, grp):
                zts.append(turn(zt, j, grp))
        consume(key, split=grp > 1 and number + 1 == len(order))
    consume(())
    return out


def solution(mesh):
    blk, _ = (mesh.shape[a] for a in AXES)
    order = plan(blk // 4)
    return jax.shard_map(
        functools.partial(shards, order),
        mesh=mesh,
        in_specs=(P(None, AXES),),
        out_specs=P(AXES, None),
        check_vma=False,
    )
```

```python
import functools
import math

import jax
import jax.numpy as jnp
from jax import lax
from jax.experimental import pallas as pl
from jax.experimental.pallas import tpu as pltpu
from jax.sharding import PartitionSpec as P


AXES = ("blk", "grp")
PLACES = {"O": 0, "X": 1, "Y": 2, "D": 3}
VMEM = pl.BlockSpec(memory_space=pltpu.VMEM)
ANY = pl.BlockSpec(memory_space=pl.ANY)
SMALL = pltpu.CompilerParams(vmem_limit_bytes=12 << 20)


def sums_kernel(r_ref, out_ref):
    summed = lax.dot_general(
        jnp.ones((8, r_ref.shape[1]), jnp.float32),
        r_ref[...],
        (((1,), (1,)), ((), ())),
        precision=lax.Precision.HIGHEST,
        preferred_element_type=jnp.float32,
    )
    for n in range(out_ref.shape[0]):
        out_ref[n] = summed[:1]


def sums(returns, devices):
    bars, width = returns.shape
    return pl.pallas_call(
        sums_kernel,
        out_shape=jax.ShapeDtypeStruct((devices, 1, bars), jnp.float32),
        in_specs=[VMEM],
        out_specs=VMEM,
        compiler_params=SMALL,
        cost_estimate=pl.CostEstimate(
            flops=bars * width, bytes_accessed=4 * bars * width, transcendentals=0
        ),
        name="sums",
    )(returns)


def stats_kernel(series, r_ref, parts_ref, z_ref, zt_ref):
    bars, width = r_ref.shape
    summed = jnp.sum(parts_ref[...], axis=0) * (1.0 / series)
    market = lax.dot_general(
        summed,
        jnp.ones((1, width), jnp.float32),
        (((0,), (0,)), ((), ())),
        precision=lax.Precision.HIGHEST,
        preferred_element_type=jnp.float32,
    )
    excess = r_ref[...] - market
    deviation = excess - jnp.sum(excess, axis=0, keepdims=True) * (1.0 / bars)
    variance = jnp.sum(deviation * deviation, axis=0, keepdims=True) * (1.0 / bars)
    z = deviation * (lax.rsqrt(variance + 1e-06) * (1.0 / math.sqrt(bars)))
    z_ref[...] = z.astype(jnp.bfloat16)
    zt_ref[...] = z.T.astype(jnp.bfloat16)


def stats(returns, parts, series):
    bars, width = returns.shape
    return pl.pallas_call(
        functools.partial(stats_kernel, series),
        out_shape=(
            jax.ShapeDtypeStruct((bars, width), jnp.bfloat16),
            jax.ShapeDtypeStruct((width, bars), jnp.bfloat16),
        ),
        in_specs=[VMEM, VMEM],
        out_specs=(VMEM, VMEM),
        compiler_params=SMALL,
        cost_estimate=pl.CostEstimate(
            flops=8 * bars * width, bytes_accessed=8 * bars * width, transcendentals=width
        ),
        name="stats",
    )(returns, parts)


def tiles_kernel(cores, keys, stack_keys, aliased, own, others, *refs):
    count = len(keys)
    blk = lax.axis_size("blk")
    b, g = (lax.axis_index(a) for a in AXES)
    refs = list(refs)
    zts = [refs.pop(0) for _ in range(cores)]
    blocks = [refs.pop(0) for _ in range(count)]
    stacks = [refs.pop(0) for _ in range(cores - 1 if stack_keys else 0)]
    if aliased:
        refs.pop(0)
    out = refs.pop(0) if own or stacks else None
    sends = [refs.pop(0) for _ in range(cores - 1)] if others else []
    tile, sems = refs
    copies = []

    def place(src, col):
        width = src.shape[1]
        copy = pltpu.make_async_copy(
            src, out.at[:, pl.ds(pl.multiple_of(col * width, width), width)], sems.at[len(copies)]
        )
        copy.start()
        copies.append(copy)

    def column(key, lane):
        k, d = key
        place = PLACES[d] ^ (3 * lax.rem(lane, 2)) if d in "XY" else PLACES[d]
        return (lax.rem(b + 4 * k, blk) ^ place) * cores + lane

    for j, stack in enumerate(stacks, 1):
        for n, key in enumerate(stack_keys):
            place(stack.at[n], column(key, lax.rem(g + cores - j, cores)))

    def product(dst, n, j):
        live = column(keys[n], g) >= b * cores + lax.rem(g + j, cores)

        @pl.when(live)
        def _():
            dst[n] = jnp.dot(
                zts[j][...], blocks[n][...], preferred_element_type=jnp.float32
            ).astype(dst.dtype)

        @pl.when(jnp.logical_not(live))
        def _():
            dst[n] = jnp.zeros(dst.shape[1:], dst.dtype)

    if own:
        for n in range(count):
            product(tile, n, 0)
            place(tile.at[n], column(keys[n], g))
    for j, send in enumerate(sends, 1):
        for n in range(count):
            product(send, n, j)
    for copy in copies:
        copy.wait()


def tiles(zts, keys, blocks, stack_keys, stacks, total, prev, own=True, others=True):
    cores, count = len(zts), len(blocks)
    height, depth = zts[0].shape
    own, others = own and count > 0, others and count > 0
    writes = own or stacks
    aliased = int(bool(writes) and prev is not None)
    placed = len(stacks) * len(stack_keys)
    out_shape, out_specs = [], []
    if writes:
        out_shape += [jax.ShapeDtypeStruct((height, total), jnp.bfloat16)]
        out_specs += [ANY]
    if others:
        out_shape += [jax.ShapeDtypeStruct((count, height, height), jnp.bfloat16)] * (cores - 1)
        out_specs += [VMEM] * (cores - 1)
    got = pl.pallas_call(
        functools.partial(tiles_kernel, cores, keys, stack_keys, aliased, own, others),
        out_shape=out_shape,
        in_specs=[VMEM] * (cores + count + len(stacks)) + [ANY] * aliased,
        out_specs=out_specs,
        scratch_shapes=[
            pltpu.VMEM((max(count * own, 1), height, height), jnp.bfloat16),
            pltpu.SemaphoreType.DMA((max(count * own + placed, 1),)),
        ],
        input_output_aliases={cores + count + len(stacks): 0} if aliased else {},
        compiler_params=SMALL,
        cost_estimate=pl.CostEstimate(
            flops=2 * max(count, 1) * (own + others) * height * depth * height + 1000,
            bytes_accessed=2 * count * (depth * height + cores * height * height),
            transcendentals=0,
        ),
    )(*zts, *blocks, *stacks, *([prev] if aliased else []))
    got = list(got)
    return got.pop(0) if writes else prev, got


TUNED = {
    4: (
        *("z1O", "x0X", ":0O", "y0Y", "z2O", "y1Y", "x1X", "y0D", ":1O,0X,0Y", "z3O", "x2X", "x1D"),
        *(":2O,1Y,1X", "y3Y", "z2Y", ":0D,3O", "y2D", "z3X", "x3D", ":2Y,2X,1D,3Y", ":2D,3X,3D"),
    )
}


def plan(depth):
    if depth in TUNED:
        key = lambda text: (int(text[:-1]), text[-1])
        return [
            (w[0], tuple(map(key, w[1:].split(","))) if w[0] == ":" else key(w[1:]))
            for w in TUNED[depth]
        ]
    lanes = {
        "z": [(k, "O") for k in range(1, depth)] + [(k, "D") for k in range(2, depth)],
        "x": [(k, "X") for k in range(depth)],
        "y": [(k, "Y") for k in range(depth)],
    }
    lanes["x"].insert(min(3, depth), (0, "D"))
    if depth > 1:
        lanes["y"].insert(2, (1, "D"))
    have = {(0, "O")}
    ready = ((0, "O"),)
    order = []
    while any(lanes.values()):
        step = []
        for link, queue in lanes.items():
            if queue and source(link, queue[0]) in have:
                step.append((link, queue.pop(0)))
        have.update(key for _, key in step)
        order += [*step, (":", ready)]
        ready = tuple(key for _, key in step)
    return [*order, (":", ready)]


def source(link, key):
    k, d = key
    if link == "z":
        return (k - 1, d)
    return (k, {"x": {"X": "O", "D": "Y"}, "y": {"Y": "O", "D": "X"}}[link].get(d))


def climb(k, depth, grp):
    top = depth - k + 1
    rest = depth - top
    pairs = []
    for p in range(depth):
        for i in range(4):
            for c in range(grp):
                if p < top:
                    to = (p - 1) % top, i, c
                elif rest > 1:
                    to = top + (p - top + 1) % rest, i, c
                else:
                    to = p, i, (c + 1) % grp
                pairs.append(((p * 4 + i) * grp + c, (to[0] * 4 + to[1]) * grp + to[2]))
    return pairs


def hop(x, link, key, blk, grp):
    if link == "z":
        return lax.ppermute(x, AXES, climb(key[0], blk // 4, grp))
    bits = {"x": (1, 2), "y": (2, 1)}[link]
    return lax.ppermute(
        x,
        AXES,
        [(i * grp + c, (i ^ bits[c % 2]) * grp + c) for i in range(blk) for c in range(grp)],
    )


def turn(x, j, grp):
    return lax.ppermute(x, "grp", [(i, (i - j) % grp) for i in range(grp)])


def shards(order, returns):
    _, width = returns.shape
    blk, grp = (lax.axis_size(a) for a in AXES)
    devices = blk * grp
    total = width * devices
    parts = lax.all_to_all(sums(returns, devices), AXES, 0, 0, tiled=True)
    z, zt = stats(returns, parts, total)
    have = {(0, "O"): z}
    zts, out, stacks, stack_keys = [zt], None, [], []

    def consume(keys, split=False):
        nonlocal out, stacks, stack_keys
        blocks = [have[key] for key in keys]
        if split:
            _, sends = tiles(zts, keys, blocks, (), [], total, None, own=False)
            out, _ = tiles(zts, keys, blocks, stack_keys, stacks, total, out, others=False)
        else:
            out, sends = tiles(zts, keys, blocks, stack_keys, stacks, total, out)
        stacks, stack_keys = [], keys
        for j, sent in enumerate(sends, 1):
            stacks.append(turn(sent, grp - j, grp))

    for number, (what, key) in enumerate(order):
        if what != ":":
            have[key] = hop(have[source(what, key)], what, key, blk, grp)
            continue
        if len(zts) < grp:
            for j in range(1, grp):
                zts.append(turn(zt, j, grp))
        consume(key, split=grp > 1 and number + 1 == len(order))
    consume(())
    return out


def solution(mesh):
    blk, _ = (mesh.shape[a] for a in AXES)
    order = plan(blk // 4)
    return jax.shard_map(
        functools.partial(shards, order),
        mesh=mesh,
        in_specs=(P(None, AXES),),
        out_specs=P(AXES, None),
        check_vma=False,
    )
```

```python
import functools
import math

import jax
import jax.numpy as jnp
from jax import lax
from jax.experimental import pallas as pl
from jax.experimental.pallas import tpu as pltpu
from jax.sharding import PartitionSpec as P


AXES = ("blk", "grp")
PLACES = {"O": 0, "X": 1, "Y": 2, "D": 3}
VMEM = pl.BlockSpec(memory_space=pltpu.VMEM)
ANY = pl.BlockSpec(memory_space=pl.ANY)
SMALL = pltpu.CompilerParams(vmem_limit_bytes=12 << 20)


def sums_kernel(r_ref, out_ref):
    summed = lax.dot_general(
        jnp.ones((8, r_ref.shape[1]), jnp.float32),
        r_ref[...],
        (((1,), (1,)), ((), ())),
        precision=lax.Precision.HIGHEST,
        preferred_element_type=jnp.float32,
    )
    for n in range(out_ref.shape[0]):
        out_ref[n] = summed[:1]


def sums(returns, devices):
    bars, width = returns.shape
    return pl.pallas_call(
        sums_kernel,
        out_shape=jax.ShapeDtypeStruct((devices, 1, bars), jnp.float32),
        in_specs=[VMEM],
        out_specs=VMEM,
        compiler_params=SMALL,
        cost_estimate=pl.CostEstimate(
            flops=bars * width, bytes_accessed=4 * bars * width, transcendentals=0
        ),
        name="sums",
    )(returns)


def stats_kernel(series, r_ref, parts_ref, z_ref):
    bars, width = r_ref.shape
    summed = jnp.sum(parts_ref[...], axis=0) * (1.0 / series)
    lanes = math.gcd(width, 128)
    market = lax.dot_general(
        summed,
        jnp.ones((1, lanes), jnp.float32),
        (((0,), (0,)), ((), ())),
        precision=lax.Precision.HIGHEST,
        preferred_element_type=jnp.float32,
    )
    market = jnp.concatenate([market] * (width // lanes), axis=1)
    excess = r_ref[...] - market
    deviation = excess - jnp.sum(excess, axis=0, keepdims=True) * (1.0 / bars)
    variance = jnp.sum(deviation * deviation, axis=0, keepdims=True) * (1.0 / bars)
    z = deviation * (lax.rsqrt(variance + 1e-06) * (1.0 / math.sqrt(bars)))
    z_ref[...] = z.astype(jnp.bfloat16)


def stats(returns, parts, series):
    bars, width = returns.shape
    return pl.pallas_call(
        functools.partial(stats_kernel, series),
        out_shape=jax.ShapeDtypeStruct((bars, width), jnp.bfloat16),
        in_specs=[VMEM, VMEM],
        out_specs=VMEM,
        compiler_params=SMALL,
        cost_estimate=pl.CostEstimate(
            flops=8 * bars * width, bytes_accessed=8 * bars * width, transcendentals=width
        ),
        name="stats",
    )(returns, parts)


def flip_kernel(z_ref, zt_ref):
    zt_ref[...] = z_ref[...].T


def flip(z):
    return pl.pallas_call(
        flip_kernel,
        out_shape=jax.ShapeDtypeStruct(z.shape[::-1], z.dtype),
        in_specs=[VMEM],
        out_specs=VMEM,
        compiler_params=SMALL,
        cost_estimate=pl.CostEstimate(
            flops=z.size, bytes_accessed=4 * z.size, transcendentals=0
        ),
        name="flip",
    )(z)


def tiles_kernel(cores, keys, stack_keys, aliased, own, others, *refs):
    count = len(keys)
    blk = lax.axis_size("blk")
    b, g = (lax.axis_index(a) for a in AXES)
    refs = list(refs)
    zts = [refs.pop(0) for _ in range(cores)]
    blocks = [refs.pop(0) for _ in range(count)]
    stacks = [refs.pop(0) for _ in range(cores - 1 if stack_keys else 0)]
    if aliased:
        refs.pop(0)
    out = refs.pop(0) if own or stacks else None
    sends = [refs.pop(0) for _ in range(cores - 1)] if others else []
    tile, sems = refs
    copies = []

    def place(src, col):
        width = src.shape[1]
        copy = pltpu.make_async_copy(
            src, out.at[:, pl.ds(pl.multiple_of(col * width, width), width)], sems.at[len(copies)]
        )
        copy.start()
        copies.append(copy)

    def column(key, lane):
        k, d = key
        place = PLACES[d] ^ (3 * lax.rem(lane, 2)) if d in "XY" else PLACES[d]
        return (lax.rem(b + 4 * k, blk) ^ place) * cores + lane

    for j, stack in enumerate(stacks, 1):
        for n, key in enumerate(stack_keys):
            place(stack.at[n], column(key, lax.rem(g + cores - j, cores)))

    def product(dst, n, j):
        live = column(keys[n], g) >= b * cores + lax.rem(g + j, cores)

        @pl.when(live)
        def _():
            dst[n] = jnp.dot(
                zts[j][...], blocks[n][...], preferred_element_type=jnp.float32
            ).astype(dst.dtype)

        @pl.when(jnp.logical_not(live))
        def _():
            dst[n] = jnp.zeros(dst.shape[1:], dst.dtype)

    if own:
        for n in range(count):
            product(tile, n, 0)
            place(tile.at[n], column(keys[n], g))
    for j, send in enumerate(sends, 1):
        for n in range(count):
            product(send, n, j)
    for copy in copies:
        copy.wait()


def tiles(zts, keys, blocks, stack_keys, stacks, total, prev, own=True, others=True):
    cores, count = len(zts), len(blocks)
    height, depth = zts[0].shape
    own, others = own and count > 0, others and count > 0
    writes = own or stacks
    aliased = int(bool(writes) and prev is not None)
    placed = len(stacks) * len(stack_keys)
    out_shape, out_specs = [], []
    if writes:
        out_shape += [jax.ShapeDtypeStruct((height, total), jnp.bfloat16)]
        out_specs += [ANY]
    if others:
        out_shape += [jax.ShapeDtypeStruct((count, height, height), jnp.bfloat16)] * (cores - 1)
        out_specs += [VMEM] * (cores - 1)
    got = pl.pallas_call(
        functools.partial(tiles_kernel, cores, keys, stack_keys, aliased, own, others),
        out_shape=out_shape,
        in_specs=[VMEM] * (cores + count + len(stacks)) + [ANY] * aliased,
        out_specs=out_specs,
        scratch_shapes=[
            pltpu.VMEM((max(count * own, 1), height, height), jnp.bfloat16),
            pltpu.SemaphoreType.DMA((max(count * own + placed, 1),)),
        ],
        input_output_aliases={cores + count + len(stacks): 0} if aliased else {},
        compiler_params=SMALL,
        cost_estimate=pl.CostEstimate(
            flops=2 * max(count, 1) * (own + others) * height * depth * height + 1000,
            bytes_accessed=2 * count * (depth * height + cores * height * height),
            transcendentals=0,
        ),
    )(*zts, *blocks, *stacks, *([prev] if aliased else []))
    got = list(got)
    return got.pop(0) if writes else prev, got


TUNED = {
    4: (
        *("z1O", "x0X", ":0O", "y0Y", "z2O", "y1Y", "x1X", "y0D", ":1O,0X,0Y", "z3O", "x2X", "x1D"),
        *(":2O,1Y,1X", "y3Y", "z2Y", ":0D,3O", "y2D", "z3X", "x3D", ":2Y,2X,1D,3Y", ":2D"),
        *(":3X,3D",),
    )
}


def plan(depth):
    if depth in TUNED:
        key = lambda text: (int(text[:-1]), text[-1])
        return [
            (w[0], tuple(map(key, w[1:].split(","))) if w[0] == ":" else key(w[1:]))
            for w in TUNED[depth]
        ]
    lanes = {
        "z": [(k, "O") for k in range(1, depth)] + [(k, "D") for k in range(2, depth)],
        "x": [(k, "X") for k in range(depth)],
        "y": [(k, "Y") for k in range(depth)],
    }
    lanes["x"].insert(min(3, depth), (0, "D"))
    if depth > 1:
        lanes["y"].insert(2, (1, "D"))
    have = {(0, "O")}
    ready = ((0, "O"),)
    order = []
    while any(lanes.values()):
        step = []
        for link, queue in lanes.items():
            if queue and source(link, queue[0]) in have:
                step.append((link, queue.pop(0)))
        have.update(key for _, key in step)
        order += [*step, (":", ready)]
        ready = tuple(key for _, key in step)
    return [*order, (":", ready)]


def source(link, key):
    k, d = key
    if link == "z":
        return (k - 1, d)
    return (k, {"x": {"X": "O", "D": "Y"}, "y": {"Y": "O", "D": "X"}}[link].get(d))


def climb(k, depth, grp):
    top = depth - k + 1
    rest = depth - top
    pairs = []
    for p in range(depth):
        for i in range(4):
            for c in range(grp):
                if p < top:
                    to = (p - 1) % top, i, c
                elif rest > 1:
                    to = top + (p - top + 1) % rest, i, c
                else:
                    to = p, i, (c + 1) % grp
                pairs.append(((p * 4 + i) * grp + c, (to[0] * 4 + to[1]) * grp + to[2]))
    return pairs


def hop(x, link, key, blk, grp):
    if link == "z":
        return lax.ppermute(x, AXES, climb(key[0], blk // 4, grp))
    bits = {"x": (1, 2), "y": (2, 1)}[link]
    return lax.ppermute(
        x,
        AXES,
        [(i * grp + c, (i ^ bits[c % 2]) * grp + c) for i in range(blk) for c in range(grp)],
    )


def turn(x, j, grp):
    return lax.ppermute(x, "grp", [(i, (i - j) % grp) for i in range(grp)])


def shards(order, returns):
    _, width = returns.shape
    blk, grp = (lax.axis_size(a) for a in AXES)
    devices = blk * grp
    total = width * devices
    parts = lax.all_to_all(sums(returns, devices), AXES, 0, 0, tiled=True)
    z = stats(returns, parts, total)
    have = {(0, "O"): z}
    zts, out, stacks, stack_keys = [], None, [], []

    def consume(keys, split=False):
        nonlocal out, stacks, stack_keys
        blocks = [have[key] for key in keys]
        if split:
            _, sends = tiles(zts, keys, blocks, (), [], total, None, own=False)
            out, _ = tiles(zts, keys, blocks, stack_keys, stacks, total, out, others=False)
        else:
            out, sends = tiles(zts, keys, blocks, stack_keys, stacks, total, out)
        stacks, stack_keys = [], keys
        for j, sent in enumerate(sends, 1):
            stacks.append(turn(sent, grp - j, grp))

    for number, (what, key) in enumerate(order):
        if what != ":":
            have[key] = hop(have[source(what, key)], what, key, blk, grp)
            continue
        if not zts:
            zts.append(flip(z))
            for j in range(1, grp):
                zts.append(turn(zts[0], j, grp))
        consume(key, split=grp > 1 and number + 1 == len(order))
    consume(())
    return out


def solution(mesh):
    blk, _ = (mesh.shape[a] for a in AXES)
    order = plan(blk // 4)
    return jax.shard_map(
        functools.partial(shards, order),
        mesh=mesh,
        in_specs=(P(None, AXES),),
        out_specs=P(AXES, None),
        check_vma=False,
    )
```

```python
import functools
import math

import jax
import jax.numpy as jnp
from jax import lax
from jax.experimental import pallas as pl
from jax.experimental.pallas import tpu as pltpu
from jax.sharding import PartitionSpec as P


AXES = ("blk", "grp")
PLACES = {"O": 0, "X": 1, "Y": 2, "D": 3}
VMEM = pl.BlockSpec(memory_space=pltpu.VMEM)
ANY = pl.BlockSpec(memory_space=pl.ANY)
SMALL = pltpu.CompilerParams(vmem_limit_bytes=12 << 20)


def sums_kernel(r_ref, out_ref):
    summed = lax.dot_general(
        jnp.ones((8, r_ref.shape[1]), jnp.float32),
        r_ref[...],
        (((1,), (1,)), ((), ())),
        precision=lax.Precision.HIGHEST,
        preferred_element_type=jnp.float32,
    )
    for n in range(out_ref.shape[0]):
        out_ref[n] = summed[:1]


def sums(returns, devices):
    bars, width = returns.shape
    return pl.pallas_call(
        sums_kernel,
        out_shape=jax.ShapeDtypeStruct((devices, 1, bars), jnp.float32),
        in_specs=[VMEM],
        out_specs=VMEM,
        compiler_params=SMALL,
        cost_estimate=pl.CostEstimate(
            flops=bars * width, bytes_accessed=4 * bars * width, transcendentals=0
        ),
        name="sums",
    )(returns)


def stats_kernel(series, r_ref, parts_ref, z_ref):
    bars, width = r_ref.shape
    summed = jnp.sum(parts_ref[...], axis=0) * (1.0 / series)
    lanes = math.gcd(width, 128)
    market = lax.dot_general(
        summed,
        jnp.ones((1, lanes), jnp.float32),
        (((0,), (0,)), ((), ())),
        precision=lax.Precision.HIGHEST,
        preferred_element_type=jnp.float32,
    )
    market = jnp.concatenate([market] * (width // lanes), axis=1)
    excess = r_ref[...] - market
    deviation = excess - jnp.sum(excess, axis=0, keepdims=True) * (1.0 / bars)
    variance = jnp.sum(deviation * deviation, axis=0, keepdims=True) * (1.0 / bars)
    z = deviation * (lax.rsqrt(variance + 1e-06) * (1.0 / math.sqrt(bars)))
    z_ref[...] = z.astype(jnp.bfloat16)


def stats(returns, parts, series):
    bars, width = returns.shape
    return pl.pallas_call(
        functools.partial(stats_kernel, series),
        out_shape=jax.ShapeDtypeStruct((bars, width), jnp.bfloat16),
        in_specs=[VMEM, VMEM],
        out_specs=VMEM,
        compiler_params=SMALL,
        cost_estimate=pl.CostEstimate(
            flops=8 * bars * width, bytes_accessed=8 * bars * width, transcendentals=width
        ),
        name="stats",
    )(returns, parts)


def flip_kernel(z_ref, zt_ref):
    zt_ref[...] = z_ref[...].T


def flip(z):
    return pl.pallas_call(
        flip_kernel,
        out_shape=jax.ShapeDtypeStruct(z.shape[::-1], z.dtype),
        in_specs=[VMEM],
        out_specs=VMEM,
        compiler_params=SMALL,
        cost_estimate=pl.CostEstimate(
            flops=z.size, bytes_accessed=4 * z.size, transcendentals=0
        ),
        name="flip",
    )(z)


def tiles_kernel(cores, keys, groups, aliased, own, others, *refs):
    count = len(keys)
    blk = lax.axis_size("blk")
    b, g = (lax.axis_index(a) for a in AXES)
    refs = list(refs)
    zts = [refs.pop(0) for _ in range(cores)]
    blocks = [refs.pop(0) for _ in range(count)]
    stacks = [[refs.pop(0) for _ in range(cores - 1)] for _ in groups]
    if aliased:
        refs.pop(0)
    out = refs.pop(0) if own or stacks else None
    sends = [refs.pop(0) for _ in range(cores - 1)] if others else []
    tile, sems = refs
    copies = []

    def place(src, col):
        width = src.shape[1]
        copy = pltpu.make_async_copy(
            src, out.at[:, pl.ds(pl.multiple_of(col * width, width), width)], sems.at[len(copies)]
        )
        copy.start()
        copies.append(copy)

    def column(key, lane):
        k, d = key
        place = PLACES[d] ^ (3 * lax.rem(lane, 2)) if d in "XY" else PLACES[d]
        return (lax.rem(b + 4 * k, blk) ^ place) * cores + lane

    for group, group_stacks in zip(groups, stacks):
        for j, stack in enumerate(group_stacks, 1):
            for n, key in enumerate(group):
                place(stack.at[n], column(key, lax.rem(g + cores - j, cores)))

    def product(dst, n, j):
        live = column(keys[n], g) >= b * cores + lax.rem(g + j, cores)

        @pl.when(live)
        def _():
            dst[n] = jnp.dot(
                zts[j][...], blocks[n][...], preferred_element_type=jnp.float32
            ).astype(dst.dtype)

        @pl.when(jnp.logical_not(live))
        def _():
            dst[n] = jnp.zeros(dst.shape[1:], dst.dtype)

    if own:
        for n in range(count):
            product(tile, n, 0)
            place(tile.at[n], column(keys[n], g))
    for j, send in enumerate(sends, 1):
        for n in range(count):
            product(send, n, j)
    for copy in copies:
        copy.wait()


def tiles(zts, keys, blocks, groups, stacks, total, prev, own=True, others=True):
    cores, count = len(zts), len(blocks)
    height, depth = zts[0].shape
    own, others = own and count > 0, others and count > 0
    writes = own or stacks
    aliased = int(bool(writes) and prev is not None)
    placed = (cores - 1) * sum(map(len, groups))
    out_shape, out_specs = [], []
    if writes:
        out_shape += [jax.ShapeDtypeStruct((height, total), jnp.bfloat16)]
        out_specs += [ANY]
    if others:
        out_shape += [jax.ShapeDtypeStruct((count, height, height), jnp.bfloat16)] * (cores - 1)
        out_specs += [VMEM] * (cores - 1)
    got = pl.pallas_call(
        functools.partial(tiles_kernel, cores, keys, tuple(groups), aliased, own, others),
        out_shape=out_shape,
        in_specs=[VMEM] * (cores + count + len(stacks)) + [ANY] * aliased,
        out_specs=out_specs,
        scratch_shapes=[
            pltpu.VMEM((max(count * own, 1), height, height), jnp.bfloat16),
            pltpu.SemaphoreType.DMA((max(count * own + placed, 1),)),
        ],
        input_output_aliases={cores + count + len(stacks): 0} if aliased else {},
        compiler_params=SMALL,
        cost_estimate=pl.CostEstimate(
            flops=2 * max(count, 1) * (own + others) * height * depth * height + 1000,
            bytes_accessed=2 * count * (depth * height + cores * height * height),
            transcendentals=0,
        ),
    )(*zts, *blocks, *stacks, *([prev] if aliased else []))
    got = list(got)
    return got.pop(0) if writes else prev, got


TUNED = {
    4: (
        *("z1O", "x0X", ":0O", "y0Y", "z2O", "y1Y", "x1X", "y0D", ":1O,0X,0Y", "z3O", "x2X", "x1D"),
        *(":2O,1Y,1X", "y3Y", "z2Y", ":0D,3O", "y2D", "z3X", "x3D", ":2Y,2X,1D,3Y", ":2D"),
        *(":3X,3D",),
    )
}


def plan(depth):
    if depth in TUNED:
        key = lambda text: (int(text[:-1]), text[-1])
        return [
            (w[0], tuple(map(key, w[1:].split(","))) if w[0] == ":" else key(w[1:]))
            for w in TUNED[depth]
        ]
    lanes = {
        "z": [(k, "O") for k in range(1, depth)] + [(k, "D") for k in range(2, depth)],
        "x": [(k, "X") for k in range(depth)],
        "y": [(k, "Y") for k in range(depth)],
    }
    lanes["x"].insert(min(3, depth), (0, "D"))
    if depth > 1:
        lanes["y"].insert(2, (1, "D"))
    have = {(0, "O")}
    ready = ((0, "O"),)
    order = []
    while any(lanes.values()):
        step = []
        for link, queue in lanes.items():
            if queue and source(link, queue[0]) in have:
                step.append((link, queue.pop(0)))
        have.update(key for _, key in step)
        order += [*step, (":", ready)]
        ready = tuple(key for _, key in step)
    return [*order, (":", ready)]


def source(link, key):
    k, d = key
    if link == "z":
        return (k - 1, d)
    return (k, {"x": {"X": "O", "D": "Y"}, "y": {"Y": "O", "D": "X"}}[link].get(d))


def climb(k, depth, grp):
    top = depth - k + 1
    rest = depth - top
    pairs = []
    for p in range(depth):
        for i in range(4):
            for c in range(grp):
                if p < top:
                    to = (p - 1) % top, i, c
                elif rest > 1:
                    to = top + (p - top + 1) % rest, i, c
                else:
                    to = p, i, (c + 1) % grp
                pairs.append(((p * 4 + i) * grp + c, (to[0] * 4 + to[1]) * grp + to[2]))
    return pairs


def hop(x, link, key, blk, grp):
    if link == "z":
        return lax.ppermute(x, AXES, climb(key[0], blk // 4, grp))
    bits = {"x": (1, 2), "y": (2, 1)}[link]
    return lax.ppermute(
        x,
        AXES,
        [(i * grp + c, (i ^ bits[c % 2]) * grp + c) for i in range(blk) for c in range(grp)],
    )


def turn(x, j, grp):
    return lax.ppermute(x, "grp", [(i, (i - j) % grp) for i in range(grp)])


def shards(order, returns):
    _, width = returns.shape
    blk, grp = (lax.axis_size(a) for a in AXES)
    devices = blk * grp
    total = width * devices
    parts = lax.all_to_all(sums(returns, devices), AXES, 0, 0, tiled=True)
    z = stats(returns, parts, total)
    have = {(0, "O"): z}
    zts, out, stacks, groups = [], None, [], []

    def consume(keys, split=False):
        nonlocal out, stacks, groups
        blocks = [have[key] for key in keys]
        if split:
            _, sends = tiles(zts, keys, blocks, (), [], total, None, own=False)
            out, _ = tiles(zts, keys, blocks, (), [], total, out, others=False)
        else:
            out, sends = tiles(zts, keys, blocks, groups, stacks, total, out)
            stacks, groups = [], []
        groups = [*groups, keys]
        for j, sent in enumerate(sends, 1):
            stacks.append(turn(sent, grp - j, grp))

    for number, (what, key) in enumerate(order):
        if what != ":":
            have[key] = hop(have[source(what, key)], what, key, blk, grp)
            continue
        if not zts:
            zts.append(flip(z))
            for j in range(1, grp):
                zts.append(turn(zts[0], j, grp))
        consume(key, split=grp > 1 and number + 1 == len(order))
    consume(())
    return out


def solution(mesh):
    blk, _ = (mesh.shape[a] for a in AXES)
    order = plan(blk // 4)
    return jax.shard_map(
        functools.partial(shards, order),
        mesh=mesh,
        in_specs=(P(None, AXES),),
        out_specs=P(AXES, None),
        check_vma=False,
    )
```
